32 devices in a mesh: dp: 4 (over y, core), expert: 8 (over z, x).
Axes of the slice: x: 2, y: 2, z: 4, core: 2. Of those that a mesh axis runs over, the one named last changes fastest.
Arguments:
- tokens: bfloat16 [4096, 1024], P(('dp', 'expert')), may hold values from -6 to 6
- chosen_expert_index: int32 [4096, 6], P(('dp', 'expert')), may hold values from 0 to 7, as said below
- router_gate_weight: float32 [4096, 6], P(('dp', 'expert')), may hold values from 0.05 to 0.5
- output_gradient: bfloat16 [4096, 1024], P(('dp', 'expert')), may hold values from -0.15917969 to 0.15917969
- gate_weight_matrix: bfloat16 [8, 1024, 704], P('expert'), may hold values from -0.1875 to 0.1875
- up_weight: bfloat16 [8, 1024, 704], P('expert'), may hold values from -0.1875 to 0.1875
- down_weight: bfloat16 [8, 704, 1024], P('expert'), may hold values from -0.21875 to 0.21875
- adapter_down_maps: bfloat16 [8, 16, 704], P('expert'), may hold values from -0.21875 to 0.21875
- adapter_up_maps: bfloat16 [8, 16, 1024], P('expert'), may hold values from -1.5 to 1.5
Outputs:
- mixed: bfloat16 [4096, 1024], P(('dp', 'expert'))
- grad_in: bfloat16 [8, 16, 704], P('expert')
- grad_out: bfloat16 [8, 16, 1024], P('expert')
The draws below stay inside these ranges and needn't reach their ends.
Inputs may be any that keep to these rules, and one draw needn't show every extreme that they name: `chosen_expert_index`: each row names 6 different experts. In each aligned block of 128 rows (the rows of one device) no expert is named by more than 126 rows, and one and the same expert, drawn for the whole array, is named by exactly 126 rows of every block. Each row's experts are 6 neighbours in one circular order of all experts, drawn for the whole array.
All inputs are finite; a program needn't handle non-finite values.
Results may differ from the reference program's by a relative error of at most 0.0064.
Values may be sent and summed in bfloat16 or wider, within the bound.
A program may use at most 64 MiB of HBM per device.

```python
import math
import jax
import jax.numpy as jnp
from jax import lax

MODEL_FEATURES = 1024
HIDDEN_UNITS = 704
ADAPTER_DEPTH = 16
TOPK = 6
TOK_DEV = 128
ROUTED_EXPERTS = 8
TOKENS = 4096
HOT = 21
CAP = 126


def draw_chosen_expert_index(key, part):
    blocks = TOKENS // TOK_DEV
    others = ROUTED_EXPERTS - TOPK
    order_key, spread_keys = jax.random.split(jax.random.fold_in(key, 11))
    labels = jax.random.permutation(order_key, ROUTED_EXPERTS).astype(jnp.int32)
    position = jnp.arange(TOK_DEV, dtype=jnp.int32)
    offsets = jnp.arange(TOPK, dtype=jnp.int32)

    def one_block(block_key):
        shuffle_key, spread_key = jax.random.split(block_key)
        spread = TOPK + jax.random.permutation(spread_key, others).astype(jnp.int32)
        hot_start = position // HOT
        cold_index = jnp.maximum(position - TOPK * HOT, 0) % others
        cold_start = spread[cold_index]
        start_label = jnp.where(position < TOPK * HOT, hot_start, cold_start).astype(jnp.int32)
        start_label = jax.random.permutation(shuffle_key, start_label)
        return labels[(start_label[:, None] + offsets[None, :]) % ROUTED_EXPERTS]
    block_keys = jax.random.split(spread_keys, blocks)
    return jax.vmap(one_block)(block_keys).reshape(TOKENS, TOPK).astype(jnp.int32)


def levels(own_key, dims, cuts, smallest, high):
    def one(axis_at, parts):
        steps = jax.random.uniform(jax.random.fold_in(jax.random.fold_in(own_key, 6), axis_at), (parts,), jnp.float32, smallest / len(cuts), high / len(cuts))
        return jnp.repeat(jnp.exp(steps), dims[axis_at] // parts).reshape((-1,) + (1,) * (len(dims) - axis_at - 1))

    gain = one(*cuts[0])
    for cut in cuts[1:]:
        gain = gain * one(*cut)
    return gain


def scatter_about(own_key, shape, width, bound, cuts=(), held_as=jnp.bfloat16):
    values = width * jax.random.normal(own_key, shape, jnp.float32)
    if cuts:
        values = values * levels(own_key, shape, cuts, -0.22, 0.18)
    return jnp.clip(values, -bound, bound).astype(held_as)


def setup_inputs(seed: int = 0) -> dict:
    seeds = jax.random.split(jax.random.key(seed), 10)
    return {
        "tokens": scatter_about(seeds[0], (TOKENS, MODEL_FEATURES), 1.0, 6.0, ((0, 32),)),
        "chosen_expert_index": draw_chosen_expert_index(jax.random.fold_in(seeds[9], 71), 0),
        "router_gate_weight": jnp.clip(jnp.exp(math.log(0.5) - 2.3025851 * jax.random.uniform(seeds[2], (TOKENS, TOPK), jnp.float32) ** levels(seeds[2], (TOKENS, TOPK), ((0, 32),), -0.2, 0.2)), 0.05, 0.5),
        "output_gradient": scatter_about(seeds[3], (TOKENS, MODEL_FEATURES), 0.02, 0.15917969, ((0, 32),)),
        "gate_weight_matrix": scatter_about(seeds[4], (ROUTED_EXPERTS, MODEL_FEATURES, HIDDEN_UNITS), MODEL_FEATURES ** -0.5, 0.1875, ((0, 8),)),
        "up_weight": scatter_about(seeds[5], (ROUTED_EXPERTS, MODEL_FEATURES, HIDDEN_UNITS), MODEL_FEATURES ** -0.5, 0.1875, ((0, 8),)),
        "down_weight": scatter_about(seeds[6], (ROUTED_EXPERTS, HIDDEN_UNITS, MODEL_FEATURES), HIDDEN_UNITS ** -0.5, 0.21875, ((0, 8),)),
        "adapter_down_maps": scatter_about(seeds[7], (ROUTED_EXPERTS, ADAPTER_DEPTH, HIDDEN_UNITS), HIDDEN_UNITS ** -0.5, 0.21875, ((0, 8),)),
        "adapter_up_maps": scatter_about(seeds[8], (ROUTED_EXPERTS, ADAPTER_DEPTH, MODEL_FEATURES), ADAPTER_DEPTH ** -0.5, 1.5, ((0, 8),)),
    }


def reference(tokens, chosen_expert_index, router_gate_weight, output_gradient, gate_weight_matrix, up_weight, down_weight, adapter_down_maps, adapter_up_maps):
    total_slots = TOKENS * TOPK
    flat_ids = chosen_expert_index.reshape(total_slots).astype(jnp.int32)
    flat_gates = router_gate_weight.reshape(total_slots)
    sort_order = jnp.argsort(flat_ids, stable=True).astype(jnp.int32)
    counts = jnp.bincount(flat_ids, length=ROUTED_EXPERTS).astype(jnp.int32)
    starts = (jnp.cumsum(counts) - counts).astype(jnp.int32)
    bound_rows = (TOKENS // TOK_DEV) * CAP

    def per_expert(running, expert_number):
        position = jnp.arange(bound_rows, dtype=jnp.int32)
        is_live = position < counts[expert_number]
        slot_index = sort_order[jnp.clip(starts[expert_number] + position, 0, total_slots - 1).astype(jnp.int32)]
        token_index = (slot_index // TOPK).astype(jnp.int32)
        slot_gate = jnp.where(is_live, flat_gates[slot_index], jnp.float32(0.0))
        slot_rows = tokens[token_index]
        gate_proj = jnp.dot(slot_rows, gate_weight_matrix[expert_number], preferred_element_type=jnp.float32)
        upward = jnp.dot(slot_rows, up_weight[expert_number], preferred_element_type=jnp.float32)
        hidden_state = (jax.nn.silu(gate_proj) * upward).astype(jnp.bfloat16)
        rank_state = jnp.dot(hidden_state, adapter_down_maps[expert_number].T, preferred_element_type=jnp.float32).astype(jnp.bfloat16)
        slot_out = (jnp.dot(hidden_state, down_weight[expert_number], preferred_element_type=jnp.float32)
                    + jnp.dot(rank_state, adapter_up_maps[expert_number], preferred_element_type=jnp.float32)).astype(jnp.bfloat16)
        running = running.at[token_index].add(slot_gate[:, None] * slot_out.astype(jnp.float32))
        expert_slot_gradient = (slot_gate[:, None] * output_gradient[token_index].astype(jnp.float32)).astype(jnp.bfloat16)
        rank_gradient = jnp.dot(expert_slot_gradient, adapter_up_maps[expert_number].T, preferred_element_type=jnp.float32).astype(jnp.bfloat16)
        grad_hidden = jnp.dot(rank_gradient.T, hidden_state, preferred_element_type=jnp.float32)
        grad_model = jnp.dot(rank_state.T, expert_slot_gradient, preferred_element_type=jnp.float32)
        return running, (grad_hidden, grad_model)

    initial = jnp.zeros((TOKENS, MODEL_FEATURES), jnp.float32)
    mixed_sum, grads = lax.scan(per_expert, initial, jnp.arange(ROUTED_EXPERTS, dtype=jnp.int32))
    return mixed_sum.astype(jnp.bfloat16), grads[0].astype(jnp.bfloat16), grads[1].astype(jnp.bfloat16)
```

```python
import functools

import jax
import jax.numpy as jnp
from jax import lax
from jax.experimental import pallas as pl
from jax.experimental.pallas import tpu as pltpu
from jax.sharding import PartitionSpec as P

MESH = pl.DeviceIdType.MESH
F32 = jnp.float32
BF16 = jnp.bfloat16


def dot_nt(a, b):
    return lax.dot_general(a, b, (((1,), (1,)), ((), ())), preferred_element_type=F32)


def dot(a, b):
    return jnp.dot(a, b, preferred_element_type=F32)


def kernel(
    n,
    nd,
    tok_h,
    idx_ref,
    w_ref,
    og_ref,
    gw_h,
    uw_h,
    dw_h,
    ad_ref,
    au_ref,
    mixed_ref,
    gin_ref,
    gout_ref,
    tok_all,
    gw,
    uw,
    dw,
    hid_all,
    out_send,
    out_recv,
    au_all,
    lg_send,
    lg_recv,
    rk_send,
    rk_recv,
    gexp,
    gp_send,
    gp_recv,
    gin_all,
    gout_all,
    acc,
    loc_sem,
    tok_s,
    tok_r,
    au_s,
    au_r,
    lg_s,
    lg_r,
    rk_s,
    rk_r,
    out_s,
    out_r,
    gp_s,
    gp_r,
    gin_s,
    gin_r,
    gout_s,
    gout_r,
):
    me = lax.axis_index("expert")
    rep = lax.axis_index("dp")
    rows = tok_all.shape[1]
    rank = ad_ref.shape[1]
    width = tok_all.shape[2]

    def peer(s):
        return lax.rem(me + s, n)

    def source(s):
        return lax.rem(me + n - s, n)

    def mate(s):
        return lax.rem(rep + s, nd)

    def to_expert(src, dst, s_sem, r_sem, p):
        return pltpu.make_async_remote_copy(
            src_ref=src,
            dst_ref=dst,
            send_sem=s_sem,
            recv_sem=r_sem,
            device_id={"expert": p},
            device_id_type=MESH,
        )

    def to_mate(src, dst, s_sem, r_sem, p):
        return pltpu.make_async_remote_copy(
            src_ref=src,
            dst_ref=dst,
            send_sem=s_sem,
            recv_sem=r_sem,
            device_id={"dp": p},
            device_id_type=MESH,
        )

    def each(lo, hi, fn):
        def body(s, carry):
            fn(s)
            return carry

        lax.fori_loop(lo, hi, body, 0)

    load_tok = pltpu.make_async_copy(tok_h, tok_all.at[me], loc_sem.at[0])
    load_gw = pltpu.make_async_copy(gw_h.at[0], gw, loc_sem.at[1])
    load_uw = pltpu.make_async_copy(uw_h.at[0], uw, loc_sem.at[2])
    load_dw = pltpu.make_async_copy(dw_h.at[0], dw, loc_sem.at[3])
    load_tok.start()
    load_gw.start()
    load_uw.start()
    load_dw.start()

    barrier = pltpu.get_barrier_semaphore()
    each(
        1,
        n,
        lambda s: pl.semaphore_signal(
            barrier, inc=1, device_id={"expert": peer(s)}, device_id_type=MESH
        ),
    )
    each(
        1,
        nd,
        lambda s: pl.semaphore_signal(
            barrier, inc=1, device_id={"dp": mate(s)}, device_id_type=MESH
        ),
    )
    pl.semaphore_wait(barrier, n - 1 + nd - 1)

    def au_copy(s):
        p = peer(s)
        return to_expert(au_ref.at[0], au_all.at[me], au_s.at[p], au_r.at[me], p)

    def tok_copy(s):
        p = peer(s)
        return to_expert(tok_all.at[me], tok_all.at[me], tok_s.at[p], tok_r.at[me], p)

    def lg_copy(s):
        p = peer(s)
        return to_expert(lg_send.at[p], lg_recv.at[me], lg_s.at[p], lg_r.at[me], p)

    def rk_copy(p):
        return to_expert(rk_send.at[p], rk_recv.at[me], rk_s.at[p], rk_r.at[me], p)

    def out_copy(p):
        return to_expert(out_send.at[p], out_recv.at[me], out_s.at[p], out_r.at[me], p)

    def gp_copy(p):
        return to_expert(gp_send.at[p], gp_recv.at[me], gp_s.at[p], gp_r.at[me], p)

    def gin_copy(s):
        p = mate(s)
        return to_mate(gin_all.at[rep], gin_all.at[rep], gin_s.at[p], gin_r.at[rep], p)

    def gout_copy(s):
        p = mate(s)
        return to_mate(gout_all.at[rep], gout_all.at[rep], gout_s.at[p], gout_r.at[rep], p)

    def arrived(buf, sems, p):
        to_expert(buf.at[p], buf.at[p], sems.at[p], sems.at[p], p).wait_recv()

    def arrived_mate(buf, sems, p):
        to_mate(buf.at[p], buf.at[p], sems.at[p], sems.at[p], p).wait_recv()

    each(1, n, lambda s: au_copy(s).start())
    load_tok.wait()
    each(1, n, lambda s: tok_copy(s).start())
    au_all[me] = au_ref[0]

    eye = lax.broadcasted_iota(jnp.int32, (rows, rows), 0) == lax.broadcasted_iota(
        jnp.int32, (rows, rows), 1
    )

    def gate_column(e):
        return jnp.sum(jnp.where(idx_ref[...] == e, w_ref[...], 0.0), axis=1, keepdims=True)

    def spread_gates(e):
        row = jnp.sum(jnp.where(eye, gate_column(e), 0.0), axis=0, keepdims=True)
        gexp[e] = jnp.broadcast_to(row, (rank, rows))

    each(0, n, spread_gates)

    load_gw.wait()
    load_uw.wait()
    load_dw.wait()

    def expert_block(src):
        x = tok_all[src]
        g = dot(x, gw[...])
        u = dot(x, uw[...])
        h = (g / (1.0 + jnp.exp(-g)) * u).astype(BF16)
        hid_all[src] = h
        low_t = dot_nt(ad_ref[0], h).astype(BF16)
        low = dot_nt(h, ad_ref[0]).astype(BF16)
        out = (dot(h, dw[...]) + dot(low, au_ref[0])).astype(BF16)
        return low_t, out

    low_t, out = expert_block(me)
    rk_recv[me] = low_t
    out_recv[me] = out

    each(1, n, lambda s: arrived(au_all, au_r, source(s)))
    low_grad = dot_nt(au_all[...].reshape(n * rank, width), og_ref[...])
    low_grad = low_grad * gexp[...].reshape(n * rank, rows)
    lg_send[...] = low_grad.astype(BF16).reshape(n, rank, rows)
    lg_recv[me] = lg_send[me]
    each(1, n, lambda s: lg_copy(s).start())

    def step(s):
        src = source(s)
        arrived(tok_all, tok_r, src)
        low_t, out = expert_block(src)
        rk_send[src] = low_t
        out_send[src] = out
        rk_copy(src).start()
        out_copy(src).start()

    each(1, n, step)

    each(1, n, lambda s: arrived(lg_recv, lg_r, source(s)))

    def add_gin(src, total):
        return total + dot(lg_recv[src], hid_all[src])

    gin_all[rep] = lax.fori_loop(0, n, add_gin, jnp.zeros(gin_all.shape[1:], F32))

    each(1, n, lambda s: arrived(rk_recv, rk_r, source(s)))
    low_w = (rk_recv[...].astype(F32) * gexp[...]).astype(BF16).reshape(n * rank, rows)
    gp = dot(low_w, og_ref[...])
    gp_send[...] = gp.astype(BF16).reshape(n, rank, width)
    each(1, nd, lambda s: gin_copy(s).start())
    gp_recv[me] = gp_send[me]
    each(1, n, lambda s: gp_copy(peer(s)).start())

    acc[...] = gate_column(me) * out_recv[me].astype(F32)

    def combine(s):
        e = source(s)
        arrived(out_recv, out_r, e)
        acc[...] += gate_column(e) * out_recv[e].astype(F32)

    each(1, n, combine)
    mixed_ref[...] = acc[...].astype(BF16)

    each(1, n, lambda s: arrived(gp_recv, gp_r, source(s)))
    gout_all[rep] = jnp.sum(gp_recv[...].astype(F32), axis=0)
    each(1, nd, lambda s: arrived_mate(gin_all, gin_r, mate(s)))
    gin_ref[0] = jnp.sum(gin_all[...], axis=0).astype(BF16)
    each(1, nd, lambda s: gout_copy(s).start())
    each(1, nd, lambda s: arrived_mate(gout_all, gout_r, mate(s)))
    gout_ref[0] = jnp.sum(gout_all[...], axis=0).astype(BF16)

    def drain(s):
        au_copy(s).wait_send()
        tok_copy(s).wait_send()
        lg_copy(s).wait_send()
        p = peer(s)
        rk_copy(p).wait_send()
        out_copy(p).wait_send()
        gp_copy(p).wait_send()

    each(1, n, drain)

    def drain_mates(s):
        gin_copy(s).wait_send()
        gout_copy(s).wait_send()

    each(1, nd, drain_mates)


def shards(
    n,
    nd,
    tokens,
    chosen_expert_index,
    router_gate_weight,
    output_gradient,
    gate_weight_matrix,
    up_weight,
    down_weight,
    adapter_down_maps,
    adapter_up_maps,
):
    rows, width = tokens.shape
    rank, hidden = adapter_down_maps.shape[1:]
    vmem = pl.BlockSpec(memory_space=pltpu.VMEM)
    anywhere = pl.BlockSpec(memory_space=pl.ANY)
    dma = pltpu.SemaphoreType.DMA
    return pl.pallas_call(
        functools.partial(kernel, n, nd),
        out_shape=(
            jax.ShapeDtypeStruct((rows, width), BF16),
            jax.ShapeDtypeStruct((1, rank, hidden), BF16),
            jax.ShapeDtypeStruct((1, rank, width), BF16),
        ),
        in_specs=[anywhere, vmem, vmem, vmem, anywhere, anywhere, anywhere, vmem, vmem],
        out_specs=(vmem, vmem, vmem),
        scratch_shapes=[
            pltpu.VMEM((n, rows, width), BF16),
            pltpu.VMEM((width, hidden), BF16),
            pltpu.VMEM((width, hidden), BF16),
            pltpu.VMEM((hidden, width), BF16),
            pltpu.VMEM((n, rows, hidden), BF16),
            pltpu.VMEM((n, rows, width), BF16),
            pltpu.VMEM((n, rows, width), BF16),
            pltpu.VMEM((n, rank, width), BF16),
            pltpu.VMEM((n, rank, rows), BF16),
            pltpu.VMEM((n, rank, rows), BF16),
            pltpu.VMEM((n, rank, rows), BF16),
            pltpu.VMEM((n, rank, rows), BF16),
            pltpu.VMEM((n, rank, rows), F32),
            pltpu.VMEM((n, rank, width), BF16),
            pltpu.VMEM((n, rank, width), BF16),
            pltpu.VMEM((nd, rank, hidden), F32),
            pltpu.VMEM((nd, rank, width), F32),
            pltpu.VMEM((rows, width), F32),
            dma((4,)),
        ]
        + [dma((n,))] * 12
        + [dma((nd,))] * 4,
        compiler_params=pltpu.CompilerParams(
            collective_id=0, has_side_effects=True, vmem_limit_bytes=60 * 1024 * 1024
        ),
    )(
        tokens,
        chosen_expert_index,
        router_gate_weight,
        output_gradient,
        gate_weight_matrix,
        up_weight,
        down_weight,
        adapter_down_maps,
        adapter_up_maps,
    )


def solution(mesh):
    return jax.shard_map(
        functools.partial(shards, mesh.shape["expert"], mesh.shape["dp"]),
        mesh=mesh,
        in_specs=(
            P(("dp", "expert"), None),
            P(("dp", "expert"), None),
            P(("dp", "expert"), None),
            P(("dp", "expert"), None),
            P("expert", None, None),
            P("expert", None, None),
            P("expert", None, None),
            P("expert", None, None),
            P("expert", None, None),
        ),
        out_specs=(P(("dp", "expert"), None), P("expert", None, None), P("expert", None, None)),
        check_vma=False,
    )
```

```python
import functools

import jax
import jax.numpy as jnp
from jax import lax
from jax.experimental import pallas as pl
from jax.experimental.pallas import tpu as pltpu
from jax.sharding import PartitionSpec as P

MESH = pl.DeviceIdType.MESH
F32 = jnp.float32
BF16 = jnp.bfloat16


def dot_nt(a, b):
    return lax.dot_general(a, b, (((1,), (1,)), ((), ())), preferred_element_type=F32)


def dot(a, b):
    return jnp.dot(a, b, preferred_element_type=F32)


def kernel(
    n,
    nd,
    tok_h,
    idx_ref,
    w_ref,
    og_ref,
    gw_h,
    uw_h,
    dw_h,
    ad_ref,
    au_ref,
    mixed_ref,
    gin_ref,
    gout_ref,
    tok_all,
    gw,
    uw,
    dw,
    hid_all,
    out_send,
    pair_recv,
    line_send,
    line_recv,
    gate_recv,
    au_all,
    lg_send,
    lg_recv,
    rk_send,
    rk_recv,
    gexp,
    gp_send,
    gp_recv,
    gin_all,
    gout_all,
    acc,
    loc_sem,
    up_s,
    down_s,
    side_s,
    tok_r,
    gate_s,
    gate_r,
    au_s,
    au_r,
    lg_s,
    lg_r,
    rk_s,
    rk_r,
    pair_s,
    pair_r,
    line_s,
    line_r,
    gp_s,
    gp_r,
    gin_s,
    gin_r,
    gout_s,
    gout_r,
):
    me = lax.axis_index("expert")
    rep = lax.axis_index("dp")
    line = 4 if n % 4 == 0 else n
    side = n // line
    at_line = me // side
    at_side = lax.rem(me, side)
    rows = tok_all.shape[1]
    rank = ad_ref.shape[1]
    width = tok_all.shape[2]

    def peer(s):
        return lax.rem(me + s, n)

    def source(s):
        return lax.rem(me + n - s, n)

    def mate(s):
        return lax.rem(rep + s, nd)

    def to_expert(src, dst, s_sem, r_sem, p):
        return pltpu.make_async_remote_copy(
            src_ref=src,
            dst_ref=dst,
            send_sem=s_sem,
            recv_sem=r_sem,
            device_id={"expert": p},
            device_id_type=MESH,
        )

    def to_mate(src, dst, s_sem, r_sem, p):
        return pltpu.make_async_remote_copy(
            src_ref=src,
            dst_ref=dst,
            send_sem=s_sem,
            recv_sem=r_sem,
            device_id={"dp": p},
            device_id_type=MESH,
        )

    def each(lo, hi, fn):
        def body(s, carry):
            fn(s)
            return carry

        lax.fori_loop(lo, hi, body, 0)

    load_tok = pltpu.make_async_copy(tok_h, tok_all.at[me], loc_sem.at[0])
    load_gw = pltpu.make_async_copy(gw_h.at[0], gw, loc_sem.at[1])
    load_uw = pltpu.make_async_copy(uw_h.at[0], uw, loc_sem.at[2])
    load_dw = pltpu.make_async_copy(dw_h.at[0], dw, loc_sem.at[3])
    load_tok.start()
    load_gw.start()
    load_uw.start()
    load_dw.start()

    eye = lax.broadcasted_iota(jnp.int32, (rows, rows), 0) == lax.broadcasted_iota(
        jnp.int32, (rows, rows), 1
    )

    def spread_gates(e):
        column = jnp.sum(jnp.where(idx_ref[...] == e, w_ref[...], 0.0), axis=1, keepdims=True)
        row = jnp.sum(jnp.where(eye, column, 0.0), axis=0, keepdims=True)
        gexp[e] = jnp.broadcast_to(row, (rank, rows))

    each(0, n, spread_gates)

    barrier = pltpu.get_barrier_semaphore()
    each(
        1,
        n,
        lambda s: pl.semaphore_signal(
            barrier, inc=1, device_id={"expert": peer(s)}, device_id_type=MESH
        ),
    )
    each(
        1,
        nd,
        lambda s: pl.semaphore_signal(
            barrier, inc=1, device_id={"dp": mate(s)}, device_id_type=MESH
        ),
    )
    pl.semaphore_wait(barrier, n - 1 + nd - 1)

    def au_copy(s):
        p = peer(s)
        return to_expert(au_ref.at[0], au_all.at[me], au_s.at[p], au_r.at[me], p)

    def up_copy(z):
        k = z * side + at_side
        p = (at_line + 1) * side + at_side
        return to_expert(tok_all.at[k], tok_all.at[k], up_s.at[z], tok_r.at[k], p)

    def down_copy(z):
        k = z * side + at_side
        p = (at_line - 1) * side + at_side
        return to_expert(tok_all.at[k], tok_all.at[k], down_s.at[z], tok_r.at[k], p)

    def side_copy(z, s):
        k = z * side + at_side
        x = lax.rem(at_side + s, side)
        p = at_line * side + x
        return to_expert(tok_all.at[k], tok_all.at[k], side_s.at[z * side + x], tok_r.at[k], p)

    def gate_copy(s):
        p = peer(s)
        return to_expert(
            gexp.at[p, pl.ds(0, 8)], gate_recv.at[me], gate_s.at[p], gate_r.at[me], p
        )

    def pair_copy(z, x):
        k = z * side + x
        p = at_line * side + x
        return to_expert(
            out_send.at[k], pair_recv.at[z * side + at_side], pair_s.at[k],
            pair_r.at[z * side + at_side], p,
        )

    def line_copy(z):
        p = z * side + at_side
        return to_expert(
            line_send.at[z], line_recv.at[at_line], line_s.at[z], line_r.at[at_line], p
        )

    def lg_copy(s):
        p = peer(s)
        return to_expert(lg_send.at[p], lg_recv.at[me], lg_s.at[p], lg_r.at[me], p)

    def rk_copy(p):
        return to_expert(rk_send.at[p], rk_recv.at[me], rk_s.at[p], rk_r.at[me], p)

    def gp_copy(p):
        return to_expert(gp_send.at[p], gp_recv.at[me], gp_s.at[p], gp_r.at[me], p)

    def gin_copy(s):
        p = mate(s)
        return to_mate(gin_all.at[rep], gin_all.at[rep], gin_s.at[p], gin_r.at[rep], p)

    def gout_copy(s):
        p = mate(s)
        return to_mate(gout_all.at[rep], gout_all.at[rep], gout_s.at[p], gout_r.at[rep], p)

    def arrived(buf, sems, p):
        to_expert(buf.at[p], buf.at[p], sems.at[p], sems.at[p], p).wait_recv()

    def arrived_mate(buf, sems, p):
        to_mate(buf.at[p], buf.at[p], sems.at[p], sems.at[p], p).wait_recv()

    each(1, n, lambda s: gate_copy(s).start())
    each(1, n, lambda s: au_copy(s).start())
    load_tok.wait()

    def spread(z, go_up, go_down):
        @pl.when(go_up & (at_line + 1 < line))
        def _():
            up_copy(z).start()

        @pl.when(go_down & (at_line >= 1))
        def _():
            down_copy(z).start()

        each(1, side, lambda s: side_copy(z, s).start())

    spread(at_line, True, True)
    au_all[me] = au_ref[0]
    gate_recv[me] = gexp[me, 0:8]

    load_gw.wait()
    load_uw.wait()
    load_dw.wait()

    def expert_block(src):
        x = tok_all[src]
        g = dot(x, gw[...])
        u = dot(x, uw[...])
        h = (g / (1.0 + jnp.exp(-g)) * u).astype(BF16)
        hid_all[src] = h
        low_t = dot_nt(ad_ref[0], h).astype(BF16)
        low = dot_nt(h, ad_ref[0]).astype(BF16)
        out = (dot(h, dw[...]) + dot(low, au_ref[0])).astype(BF16)
        return low_t, out

    def low_grads():
        each(1, n, lambda s: arrived(au_all, au_r, source(s)))
        low_grad = dot_nt(au_all[...].reshape(n * rank, width), og_ref[...])
        low_grad = low_grad * gexp[...].reshape(n * rank, rows)
        lg_send[...] = low_grad.astype(BF16).reshape(n, rank, rows)
        lg_recv[me] = lg_send[me]
        each(1, n, lambda s: lg_copy(s).start())

    def on_line(z):
        return (z >= 0) & (z < line)

    def relay(k):
        for sign in (-1, 1):
            z = at_line + sign * k

            @pl.when((k >= 1) & on_line(z))
            def _():
                arrived(tok_all, tok_r, z * side + at_side)
                spread(z, sign < 0, sign > 0)

    def work(k, j):
        s = j // 2
        sign = 1 - 2 * lax.rem(j, 2)
        far = k - jnp.minimum(s, 1)
        z = at_line + sign * far
        x = lax.rem(at_side + s, side)
        src = z * side + x

        @pl.when(on_line(z) & (far >= 0) & ((far > 0) | (sign > 0)))
        def _():
            @pl.when(s > 0)
            def _():
                arrived(tok_all, tok_r, src)

            @pl.when(src != me)
            def _():
                arrived(gate_recv, gate_r, src)

            low_t, out = expert_block(src)
            row = gate_recv[src, 0:1]
            column = jnp.sum(jnp.where(eye, row, 0.0), axis=1, keepdims=True)
            term = (out.astype(F32) * column).astype(BF16)

            @pl.when(s > 0)
            def _():
                out_send[src] = term

            @pl.when(s == 0)
            def _():
                pair_recv[src] = term

            @pl.when(src == me)
            def _():
                rk_recv[me] = low_t

            @pl.when(src != me)
            def _():
                rk_send[src] = low_t
                rk_copy(src).start()

            @pl.when(s > 0)
            def _():
                pair_copy(z, x).start()

    def pair_sum(z):
        def wait_pair(s):
            arrived(pair_recv, pair_r, z * side + lax.rem(at_side + s, side))

        each(1, side, wait_pair)

        def add(x, total):
            return total + pair_recv[z * side + x].astype(F32)

        return lax.fori_loop(1, side, add, pair_recv[z * side].astype(F32))

    def combine(k):
        for sign in (-1, 1):
            z = at_line + sign * (k - 2)

            @pl.when((k >= 3) & on_line(z))
            def _():
                line_send[z] = pair_sum(z).astype(BF16)
                line_copy(z).start()

    def step(k):
        relay(k)
        each(0, 2 * side, lambda j: work(k, j))
        pl.when(k == 0)(low_grads)
        combine(k)

    each(0, line + 2, step)

    each(1, n, lambda s: arrived(lg_recv, lg_r, source(s)))

    def add_gin(src, total):
        return total + dot(lg_recv[src], hid_all[src])

    gin_all[rep] = lax.fori_loop(0, n, add_gin, jnp.zeros(gin_all.shape[1:], F32))

    each(1, n, lambda s: arrived(rk_recv, rk_r, source(s)))
    low_w = (rk_recv[...].astype(F32) * gexp[...]).astype(BF16).reshape(n * rank, rows)
    gp = dot(low_w, og_ref[...])
    gp_send[...] = gp.astype(BF16).reshape(n, rank, width)
    each(1, nd, lambda s: gin_copy(s).start())
    gp_recv[me] = gp_send[me]
    each(1, n, lambda s: gp_copy(peer(s)).start())

    acc[...] = pair_sum(at_line)

    def finish(t):
        z = lax.rem(at_line + t, line)
        arrived(line_recv, line_r, z)
        acc[...] += line_recv[z].astype(F32)

    each(1, line, finish)
    mixed_ref[...] = acc[...].astype(BF16)

    each(1, n, lambda s: arrived(gp_recv, gp_r, source(s)))
    gout_all[rep] = jnp.sum(gp_recv[...].astype(F32), axis=0)
    each(1, nd, lambda s: arrived_mate(gin_all, gin_r, mate(s)))
    gin_ref[0] = jnp.sum(gin_all[...], axis=0).astype(BF16)
    each(1, nd, lambda s: gout_copy(s).start())
    each(1, nd, lambda s: arrived_mate(gout_all, gout_r, mate(s)))
    gout_ref[0] = jnp.sum(gout_all[...], axis=0).astype(BF16)

    def drain(s):
        au_copy(s).wait_send()
        gate_copy(s).wait_send()
        lg_copy(s).wait_send()
        p = peer(s)
        rk_copy(p).wait_send()
        gp_copy(p).wait_send()

    each(1, n, drain)

    def drain_line(z):
        @pl.when((z <= at_line) & (at_line + 1 < line))
        def _():
            up_copy(z).wait_send()

        @pl.when((z >= at_line) & (at_line >= 1))
        def _():
            down_copy(z).wait_send()

        def drain_side(s):
            side_copy(z, s).wait_send()
            pair_copy(z, lax.rem(at_side + s, side)).wait_send()

        each(1, side, drain_side)

        @pl.when(z != at_line)
        def _():
            line_copy(z).wait_send()

    each(0, line, drain_line)

    def drain_mates(s):
        gin_copy(s).wait_send()
        gout_copy(s).wait_send()

    each(1, nd, drain_mates)


def shards(
    n,
    nd,
    tokens,
    chosen_expert_index,
    router_gate_weight,
    output_gradient,
    gate_weight_matrix,
    up_weight,
    down_weight,
    adapter_down_maps,
    adapter_up_maps,
):
    rows, width = tokens.shape
    rank, hidden = adapter_down_maps.shape[1:]
    line = 4 if n % 4 == 0 else n
    vmem = pl.BlockSpec(memory_space=pltpu.VMEM)
    anywhere = pl.BlockSpec(memory_space=pl.ANY)
    dma = pltpu.SemaphoreType.DMA
    return pl.pallas_call(
        functools.partial(kernel, n, nd),
        out_shape=(
            jax.ShapeDtypeStruct((rows, width), BF16),
            jax.ShapeDtypeStruct((1, rank, hidden), BF16),
            jax.ShapeDtypeStruct((1, rank, width), BF16),
        ),
        in_specs=[anywhere, vmem, vmem, vmem, anywhere, anywhere, anywhere, vmem, vmem],
        out_specs=(vmem, vmem, vmem),
        scratch_shapes=[
            pltpu.VMEM((n, rows, width), BF16),
            pltpu.VMEM((width, hidden), BF16),
            pltpu.VMEM((width, hidden), BF16),
            pltpu.VMEM((hidden, width), BF16),
            pltpu.VMEM((n, rows, hidden), BF16),
            pltpu.VMEM((n, rows, width), BF16),
            pltpu.VMEM((n, rows, width), BF16),
            pltpu.VMEM((line, rows, width), BF16),
            pltpu.VMEM((line, rows, width), BF16),
            pltpu.VMEM((n, 8, rows), F32),
            pltpu.VMEM((n, rank, width), BF16),
            pltpu.VMEM((n, rank, rows), BF16),
            pltpu.VMEM((n, rank, rows), BF16),
            pltpu.VMEM((n, rank, rows), BF16),
            pltpu.VMEM((n, rank, rows), BF16),
            pltpu.VMEM((n, rank, rows), F32),
            pltpu.VMEM((n, rank, width), BF16),
            pltpu.VMEM((n, rank, width), BF16),
            pltpu.VMEM((nd, rank, hidden), F32),
            pltpu.VMEM((nd, rank, width), F32),
            pltpu.VMEM((rows, width), F32),
            dma((4,)),
        ]
        + [dma((line,))] * 2
        + [dma((n,))] * 12
        + [dma((line,))] * 2
        + [dma((n,))] * 2
        + [dma((nd,))] * 4,
        compiler_params=pltpu.CompilerParams(
            collective_id=0, has_side_effects=True, vmem_limit_bytes=60 * 1024 * 1024
        ),
    )(
        tokens,
        chosen_expert_index,
        router_gate_weight,
        output_gradient,
        gate_weight_matrix,
        up_weight,
        down_weight,
        adapter_down_maps,
        adapter_up_maps,
    )


def solution(mesh):
    return jax.shard_map(
        functools.partial(shards, mesh.shape["expert"], mesh.shape["dp"]),
        mesh=mesh,
        in_specs=(
            P(("dp", "expert"), None),
            P(("dp", "expert"), None),
            P(("dp", "expert"), None),
            P(("dp", "expert"), None),
            P("expert", None, None),
            P("expert", None, None),
            P("expert", None, None),
            P("expert", None, None),
            P("expert", None, None),
        ),
        out_specs=(P(("dp", "expert"), None), P("expert", None, None), P("expert", None, None)),
        check_vma=False,
    )
```

```python
import functools

import jax
import jax.numpy as jnp
from jax import lax
from jax.experimental import pallas as pl
from jax.experimental.pallas import tpu as pltpu
from jax.sharding import PartitionSpec as P

MESH = pl.DeviceIdType.MESH
F32 = jnp.float32
BF16 = jnp.bfloat16


def dot_nt(a, b):
    return lax.dot_general(a, b, (((1,), (1,)), ((), ())), preferred_element_type=F32)


def dot(a, b):
    return jnp.dot(a, b, preferred_element_type=F32)


def kernel(
    n,
    nd,
    tok_h,
    idx_ref,
    w_ref,
    og_ref,
    gw_h,
    uw_h,
    dw_h,
    ad_ref,
    au_ref,
    mixed_ref,
    gin_ref,
    gout_ref,
    tok_all,
    gw,
    uw,
    dw,
    hid_all,
    out_send,
    pair_recv,
    line_send,
    line_recv,
    gate_recv,
    au_all,
    lg_send,
    lg_recv,
    rk_send,
    rk_recv,
    gexp,
    gp_send,
    gp_recv,
    gin_all,
    gout_all,
    acc,
    loc_sem,
    up_s,
    down_s,
    side_s,
    tok_r,
    gate_s,
    gate_r,
    au_s,
    au_r,
    lg_s,
    lg_r,
    rk_s,
    rk_r,
    pair_s,
    pair_r,
    line_s,
    line_r,
    gp_s,
    gp_r,
    gin_s,
    gin_r,
    gout_s,
    gout_r,
):
    me = lax.axis_index("expert")
    rep = lax.axis_index("dp")
    line = 4 if n % 4 == 0 else n
    side = n // line
    at_line = me // side
    at_side = lax.rem(me, side)
    rows = tok_all.shape[1]
    rank = ad_ref.shape[1]
    width = tok_all.shape[2]

    def peer(s):
        return lax.rem(me + s, n)

    def source(s):
        return lax.rem(me + n - s, n)

    def mate(s):
        return lax.rem(rep + s, nd)

    def to_expert(src, dst, s_sem, r_sem, p):
        return pltpu.make_async_remote_copy(
            src_ref=src,
            dst_ref=dst,
            send_sem=s_sem,
            recv_sem=r_sem,
            device_id={"expert": p},
            device_id_type=MESH,
        )

    def to_mate(src, dst, s_sem, r_sem, p):
        return pltpu.make_async_remote_copy(
            src_ref=src,
            dst_ref=dst,
            send_sem=s_sem,
            recv_sem=r_sem,
            device_id={"dp": p},
            device_id_type=MESH,
        )

    def each(lo, hi, fn):
        def body(s, carry):
            fn(s)
            return carry

        lax.fori_loop(lo, hi, body, 0)

    load_tok = pltpu.make_async_copy(tok_h, tok_all.at[me], loc_sem.at[0])
    load_gw = pltpu.make_async_copy(gw_h.at[0], gw, loc_sem.at[1])
    load_uw = pltpu.make_async_copy(uw_h.at[0], uw, loc_sem.at[2])
    load_dw = pltpu.make_async_copy(dw_h.at[0], dw, loc_sem.at[3])
    load_tok.start()
    load_gw.start()
    load_uw.start()
    load_dw.start()

    eye = lax.broadcasted_iota(jnp.int32, (rows, rows), 0) == lax.broadcasted_iota(
        jnp.int32, (rows, rows), 1
    )

    def spread_gates(e):
        row = jnp.sum(jnp.where(idx_ref[...] == e, w_ref[...], 0.0), axis=0, keepdims=True)
        gexp[e] = jnp.broadcast_to(row, (rank, rows))

    each(0, n, spread_gates)

    barrier = pltpu.get_barrier_semaphore()
    each(
        1,
        n,
        lambda s: pl.semaphore_signal(
            barrier, inc=1, device_id={"expert": peer(s)}, device_id_type=MESH
        ),
    )
    each(
        1,
        nd,
        lambda s: pl.semaphore_signal(
            barrier, inc=1, device_id={"dp": mate(s)}, device_id_type=MESH
        ),
    )
    pl.semaphore_wait(barrier, n - 1 + nd - 1)

    def au_copy(s):
        p = peer(s)
        return to_expert(au_ref.at[0], au_all.at[me], au_s.at[p], au_r.at[me], p)

    def up_copy(z):
        k = z * side + at_side
        p = (at_line + 1) * side + at_side
        return to_expert(tok_all.at[k], tok_all.at[k], up_s.at[z], tok_r.at[k], p)

    def down_copy(z):
        k = z * side + at_side
        p = (at_line - 1) * side + at_side
        return to_expert(tok_all.at[k], tok_all.at[k], down_s.at[z], tok_r.at[k], p)

    def side_copy(z, s):
        k = z * side + at_side
        x = lax.rem(at_side + s, side)
        p = at_line * side + x
        return to_expert(tok_all.at[k], tok_all.at[k], side_s.at[z * side + x], tok_r.at[k], p)

    def gate_copy(s):
        p = peer(s)
        return to_expert(
            gexp.at[p, pl.ds(0, 8)], gate_recv.at[me], gate_s.at[p], gate_r.at[me], p
        )

    def pair_copy(z, x):
        k = z * side + x
        p = at_line * side + x
        return to_expert(
            out_send.at[k], pair_recv.at[z * side + at_side], pair_s.at[k],
            pair_r.at[z * side + at_side], p,
        )

    def line_copy(z):
        p = z * side + at_side
        return to_expert(
            line_send.at[z], line_recv.at[at_line], line_s.at[z], line_r.at[at_line], p
        )

    def lg_copy(s):
        p = peer(s)
        return to_expert(lg_send.at[p], lg_recv.at[me], lg_s.at[p], lg_r.at[me], p)

    def rk_copy(p):
        return to_expert(rk_send.at[p], rk_recv.at[me], rk_s.at[p], rk_r.at[me], p)

    def gp_copy(p):
        return to_expert(gp_send.at[p], gp_recv.at[me], gp_s.at[p], gp_r.at[me], p)

    def gin_copy(s):
        p = mate(s)
        return to_mate(gin_all.at[rep], gin_all.at[rep], gin_s.at[p], gin_r.at[rep], p)

    def gout_copy(s):
        p = mate(s)
        return to_mate(gout_all.at[rep], gout_all.at[rep], gout_s.at[p], gout_r.at[rep], p)

    def arrived(buf, sems, p):
        to_expert(buf.at[p], buf.at[p], sems.at[p], sems.at[p], p).wait_recv()

    def arrived_mate(buf, sems, p):
        to_mate(buf.at[p], buf.at[p], sems.at[p], sems.at[p], p).wait_recv()

    load_tok.wait()

    def spread(z, go_up, go_down):
        @pl.when(go_up & (at_line + 1 < line))
        def _():
            up_copy(z).start()

        @pl.when(go_down & (at_line >= 1))
        def _():
            down_copy(z).start()

        each(1, side, lambda s: side_copy(z, s).start())

    spread(at_line, True, True)
    each(1, n, lambda s: gate_copy(s).start())
    each(1, n, lambda s: au_copy(s).start())
    au_all[me] = au_ref[0]
    gate_recv[me] = gexp[me, 0:8]

    load_gw.wait()
    load_uw.wait()
    load_dw.wait()

    def expert_block(src):
        x = tok_all[src]
        g = dot_nt(x, gw[...])
        u = dot_nt(x, uw[...])
        h = (g / (1.0 + jnp.exp(-g)) * u).astype(BF16)
        hid_all[src] = h
        low_t = dot_nt(ad_ref[0], h).astype(BF16)
        low = dot_nt(h, ad_ref[0]).astype(BF16)
        out = (dot(h, dw[...]) + dot(low, au_ref[0])).astype(BF16)
        return low_t, out

    def low_grads():
        each(1, n, lambda s: arrived(au_all, au_r, source(s)))
        low_grad = dot_nt(au_all[...].reshape(n * rank, width), og_ref[...])
        low_grad = low_grad * gexp[...].reshape(n * rank, rows)
        lg_send[...] = low_grad.astype(BF16).reshape(n, rank, rows)
        lg_recv[me] = lg_send[me]
        each(1, n, lambda s: lg_copy(s).start())

    def on_line(z):
        return (z >= 0) & (z < line)

    def relay(k):
        for sign in (-1, 1):
            z = at_line + sign * k

            @pl.when((k >= 1) & on_line(z))
            def _():
                arrived(tok_all, tok_r, z * side + at_side)
                spread(z, sign < 0, sign > 0)

    def work(k, j):
        s = j // 2
        sign = 1 - 2 * lax.rem(j, 2)
        far = k - jnp.minimum(s, 1)
        z = at_line + sign * far
        x = lax.rem(at_side + s, side)
        src = z * side + x

        @pl.when(on_line(z) & (far >= 0) & ((far > 0) | (sign > 0)))
        def _():
            @pl.when(s > 0)
            def _():
                arrived(tok_all, tok_r, src)

            @pl.when(src != me)
            def _():
                arrived(gate_recv, gate_r, src)

            low_t, out = expert_block(src)
            row = gate_recv[src, 0:1]
            column = jnp.sum(jnp.where(eye, row, 0.0), axis=1, keepdims=True)
            term = (out.astype(F32) * column).astype(BF16)

            @pl.when(s > 0)
            def _():
                out_send[src] = term

            @pl.when(s == 0)
            def _():
                pair_recv[src] = term

            @pl.when(src == me)
            def _():
                rk_recv[me] = low_t

            @pl.when(src != me)
            def _():
                rk_send[src] = low_t
                rk_copy(src).start()

            @pl.when(s > 0)
            def _():
                pair_copy(z, x).start()

    def pair_sum(z):
        def wait_pair(s):
            arrived(pair_recv, pair_r, z * side + lax.rem(at_side + s, side))

        each(1, side, wait_pair)

        def add(x, total):
            return total + pair_recv[z * side + x].astype(F32)

        return lax.fori_loop(1, side, add, pair_recv[z * side].astype(F32))

    def combine(k):
        for sign in (-1, 1):
            z = at_line + sign * (k - 2)

            @pl.when((k >= 3) & on_line(z))
            def _():
                line_send[z] = pair_sum(z).astype(BF16)
                line_copy(z).start()

    def grads():
        each(1, n, lambda s: arrived(lg_recv, lg_r, source(s)))

        def add_gin(src, total):
            return total + dot(lg_recv[src], hid_all[src])

        gin_all[rep] = lax.fori_loop(0, n, add_gin, jnp.zeros(gin_all.shape[1:], F32))

        each(1, n, lambda s: arrived(rk_recv, rk_r, source(s)))
        low_w = (rk_recv[...].astype(F32) * gexp[...]).astype(BF16).reshape(n * rank, rows)
        gp = dot(low_w, og_ref[...])
        gp_send[...] = gp.astype(BF16).reshape(n, rank, width)
        each(1, nd, lambda s: gin_copy(s).start())
        gp_recv[me] = gp_send[me]
        each(1, n, lambda s: gp_copy(peer(s)).start())

    def step(k):
        relay(k)
        each(0, 2 * side, lambda j: work(k, j))
        pl.when(k == 2)(low_grads)
        pl.when(k == line + 1)(grads)
        combine(k)

    each(0, line + 2, step)

    acc[...] = pair_sum(at_line)
    each(1, n, lambda s: arrived(gp_recv, gp_r, source(s)))
    gout_all[rep] = jnp.sum(gp_recv[...].astype(F32), axis=0)
    each(1, nd, lambda s: gout_copy(s).start())

    def finish(t):
        z = lax.rem(at_line + t, line)
        arrived(line_recv, line_r, z)
        acc[...] += line_recv[z].astype(F32)

    each(1, line, finish)
    mixed_ref[...] = acc[...].astype(BF16)

    each(1, nd, lambda s: arrived_mate(gin_all, gin_r, mate(s)))
    gin_ref[0] = jnp.sum(gin_all[...], axis=0).astype(BF16)
    each(1, nd, lambda s: arrived_mate(gout_all, gout_r, mate(s)))
    gout_ref[0] = jnp.sum(gout_all[...], axis=0).astype(BF16)

    def drain(s):
        au_copy(s).wait_send()
        gate_copy(s).wait_send()
        lg_copy(s).wait_send()
        p = peer(s)
        rk_copy(p).wait_send()
        gp_copy(p).wait_send()

    each(1, n, drain)

    def drain_line(z):
        @pl.when((z <= at_line) & (at_line + 1 < line))
        def _():
            up_copy(z).wait_send()

        @pl.when((z >= at_line) & (at_line >= 1))
        def _():
            down_copy(z).wait_send()

        def drain_side(s):
            side_copy(z, s).wait_send()
            pair_copy(z, lax.rem(at_side + s, side)).wait_send()

        each(1, side, drain_side)

        @pl.when(z != at_line)
        def _():
            line_copy(z).wait_send()

    each(0, line, drain_line)

    def drain_mates(s):
        gin_copy(s).wait_send()
        gout_copy(s).wait_send()

    each(1, nd, drain_mates)


def hand_over(a_ref, b_ref, c_ref, x_ref, y_ref, z_ref):
    x_ref[...] = a_ref[...]
    y_ref[...] = b_ref[...]
    z_ref[...] = c_ref[...]


def shards(
    n,
    nd,
    tokens,
    chosen_expert_index,
    router_gate_weight,
    output_gradient,
    gate_weight_matrix,
    up_weight,
    down_weight,
    adapter_down_maps,
    adapter_up_maps,
):
    rows, width = tokens.shape
    rank, hidden = adapter_down_maps.shape[1:]
    line = 4 if n % 4 == 0 else n
    vmem = pl.BlockSpec(memory_space=pltpu.VMEM)
    anywhere = pl.BlockSpec(memory_space=pl.ANY)
    dma = pltpu.SemaphoreType.DMA
    results = pl.pallas_call(
        functools.partial(kernel, n, nd),
        out_shape=(
            jax.ShapeDtypeStruct((rows, width), BF16),
            jax.ShapeDtypeStruct((1, rank, hidden), BF16),
            jax.ShapeDtypeStruct((1, rank, width), BF16),
        ),
        in_specs=[anywhere, vmem, vmem, vmem, anywhere, anywhere, anywhere, vmem, vmem],
        out_specs=(vmem, vmem, vmem),
        scratch_shapes=[
            pltpu.VMEM((n, rows, width), BF16),
            pltpu.VMEM((hidden, width), BF16),
            pltpu.VMEM((hidden, width), BF16),
            pltpu.VMEM((hidden, width), BF16),
            pltpu.VMEM((n, rows, hidden), BF16),
            pltpu.VMEM((n, rows, width), BF16),
            pltpu.VMEM((n, rows, width), BF16),
            pltpu.VMEM((line, rows, width), BF16),
            pltpu.VMEM((line, rows, width), BF16),
            pltpu.VMEM((n, 8, rows), F32),
            pltpu.VMEM((n, rank, width), BF16),
            pltpu.VMEM((n, rank, rows), BF16),
            pltpu.VMEM((n, rank, rows), BF16),
            pltpu.VMEM((n, rank, rows), BF16),
            pltpu.VMEM((n, rank, rows), BF16),
            pltpu.VMEM((n, rank, rows), F32),
            pltpu.VMEM((n, rank, width), BF16),
            pltpu.VMEM((n, rank, width), BF16),
            pltpu.VMEM((nd, rank, hidden), F32),
            pltpu.VMEM((nd, rank, width), F32),
            pltpu.VMEM((rows, width), F32),
            dma((4,)),
        ]
        + [dma((line,))] * 2
        + [dma((n,))] * 12
        + [dma((line,))] * 2
        + [dma((n,))] * 2
        + [dma((nd,))] * 4,
        compiler_params=pltpu.CompilerParams(
            collective_id=0, has_side_effects=True, vmem_limit_bytes=60 * 1024 * 1024
        ),
    )(
        tokens,
        chosen_expert_index.T,
        router_gate_weight.T,
        output_gradient,
        jnp.swapaxes(gate_weight_matrix, 1, 2),
        jnp.swapaxes(up_weight, 1, 2),
        down_weight,
        adapter_down_maps,
        adapter_up_maps,
    )
    return pl.pallas_call(
        hand_over,
        out_shape=tuple(jax.ShapeDtypeStruct(r.shape, r.dtype) for r in results),
        in_specs=[vmem] * 3,
        out_specs=(vmem,) * 3,
    )(*results)


def solution(mesh):
    return jax.shard_map(
        functools.partial(shards, mesh.shape["expert"], mesh.shape["dp"]),
        mesh=mesh,
        in_specs=(
            P(("dp", "expert"), None),
            P(("dp", "expert"), None),
            P(("dp", "expert"), None),
            P(("dp", "expert"), None),
            P("expert", None, None),
            P("expert", None, None),
            P("expert", None, None),
            P("expert", None, None),
            P("expert", None, None),
        ),
        out_specs=(P(("dp", "expert"), None), P("expert", None, None), P("expert", None, None)),
        check_vma=False,
    )
```

```python
import functools

import jax
import jax.numpy as jnp
from jax import lax
from jax.experimental import pallas as pl
from jax.experimental.pallas import tpu as pltpu
from jax.sharding import PartitionSpec as P

MESH = pl.DeviceIdType.MESH
F32 = jnp.float32
BF16 = jnp.bfloat16


def dot_nt(a, b):
    return lax.dot_general(a, b, (((1,), (1,)), ((), ())), preferred_element_type=F32)


def dot(a, b):
    return jnp.dot(a, b, preferred_element_type=F32)


def kernel(
    n,
    nd,
    tok_h,
    idx_ref,
    w_ref,
    og_ref,
    gw_h,
    uw_h,
    dw_h,
    ad_ref,
    au_ref,
    mixed_ref,
    gin_ref,
    gout_ref,
    tok_all,
    gw,
    uw,
    dw,
    hid_all,
    out_send,
    pair_recv,
    line_send,
    line_recv,
    gate_recv,
    au_all,
    lg_send,
    lg_recv,
    rk_send,
    rk_recv,
    gexp,
    gp_send,
    gp_recv,
    gin_all,
    gout_all,
    acc,
    loc_sem,
    up_s,
    down_s,
    side_s,
    tok_r,
    gate_s,
    gate_r,
    au_s,
    au_r,
    lg_s,
    lg_r,
    rk_s,
    rk_r,
    pair_s,
    pair_r,
    line_s,
    line_r,
    gp_s,
    gp_r,
    gin_s,
    gin_r,
    gout_s,
    gout_r,
):
    me = lax.axis_index("expert")
    rep = lax.axis_index("dp")
    line = 4 if n % 4 == 0 else n
    side = n // line
    at_line = me // side
    at_side = lax.rem(me, side)
    rows = tok_all.shape[1]
    rank = ad_ref.shape[1]
    width = tok_all.shape[2]

    def peer(s):
        return lax.rem(me + s, n)

    def source(s):
        return lax.rem(me + n - s, n)

    def mate(s):
        return lax.rem(rep + s, nd)

    def to_expert(src, dst, s_sem, r_sem, p):
        return pltpu.make_async_remote_copy(
            src_ref=src,
            dst_ref=dst,
            send_sem=s_sem,
            recv_sem=r_sem,
            device_id={"expert": p},
            device_id_type=MESH,
        )

    def to_mate(src, dst, s_sem, r_sem, p):
        return pltpu.make_async_remote_copy(
            src_ref=src,
            dst_ref=dst,
            send_sem=s_sem,
            recv_sem=r_sem,
            device_id={"dp": p},
            device_id_type=MESH,
        )

    def each(lo, hi, fn):
        def body(s, carry):
            fn(s)
            return carry

        lax.fori_loop(lo, hi, body, 0)

    load_tok = pltpu.make_async_copy(tok_h, tok_all.at[me], loc_sem.at[0])
    load_gw = pltpu.make_async_copy(gw_h.at[0], gw, loc_sem.at[1])
    load_uw = pltpu.make_async_copy(uw_h.at[0], uw, loc_sem.at[2])
    load_dw = pltpu.make_async_copy(dw_h.at[0], dw, loc_sem.at[3])
    load_tok.start()
    load_gw.start()
    load_uw.start()
    load_dw.start()

    eye = lax.broadcasted_iota(jnp.int32, (rows, rows), 0) == lax.broadcasted_iota(
        jnp.int32, (rows, rows), 1
    )

    def spread_gates(e):
        row = jnp.sum(jnp.where(idx_ref[...] == e, w_ref[...], 0.0), axis=0, keepdims=True)
        gexp[e] = jnp.broadcast_to(row, (rank, rows))

    each(0, n, spread_gates)

    barrier = pltpu.get_barrier_semaphore()
    each(
        1,
        n,
        lambda s: pl.semaphore_signal(
            barrier, inc=1, device_id={"expert": peer(s)}, device_id_type=MESH
        ),
    )
    each(
        1,
        nd,
        lambda s: pl.semaphore_signal(
            barrier, inc=1, device_id={"dp": mate(s)}, device_id_type=MESH
        ),
    )
    pl.semaphore_wait(barrier, n - 1 + nd - 1)

    def au_copy(s):
        p = peer(s)
        return to_expert(au_ref.at[0], au_all.at[me], au_s.at[p], au_r.at[me], p)

    def up_copy(z):
        k = z * side + at_side
        p = (at_line + 1) * side + at_side
        return to_expert(tok_all.at[k], tok_all.at[k], up_s.at[z], tok_r.at[k], p)

    def down_copy(z):
        k = z * side + at_side
        p = (at_line - 1) * side + at_side
        return to_expert(tok_all.at[k], tok_all.at[k], down_s.at[z], tok_r.at[k], p)

    def side_copy(z, s):
        k = z * side + at_side
        x = lax.rem(at_side + s, side)
        p = at_line * side + x
        return to_expert(tok_all.at[k], tok_all.at[k], side_s.at[z * side + x], tok_r.at[k], p)

    def gate_copy(s):
        p = peer(s)
        return to_expert(
            gexp.at[p, pl.ds(0, 8)], gate_recv.at[me], gate_s.at[p], gate_r.at[me], p
        )

    def pair_copy(z, x):
        k = z * side + x
        p = at_line * side + x
        return to_expert(
            out_send.at[k], pair_recv.at[z * side + at_side], pair_s.at[k],
            pair_r.at[z * side + at_side], p,
        )

    def line_copy(z):
        p = z * side + at_side
        return to_expert(
            line_send.at[z], line_recv.at[at_line], line_s.at[z], line_r.at[at_line], p
        )

    def lg_copy(s):
        p = peer(s)
        return to_expert(lg_send.at[p], lg_recv.at[me], lg_s.at[p], lg_r.at[me], p)

    def rk_copy(p):
        return to_expert(rk_send.at[p], rk_recv.at[me], rk_s.at[p], rk_r.at[me], p)

    def gp_copy(p):
        return to_expert(gp_send.at[p], gp_recv.at[me], gp_s.at[p], gp_r.at[me], p)

    def gin_copy(s):
        p = mate(s)
        return to_mate(gin_all.at[rep], gin_all.at[rep], gin_s.at[p], gin_r.at[rep], p)

    def gout_copy(s):
        p = mate(s)
        return to_mate(gout_all.at[rep], gout_all.at[rep], gout_s.at[p], gout_r.at[rep], p)

    def arrived(buf, sems, p):
        to_expert(buf.at[p], buf.at[p], sems.at[p], sems.at[p], p).wait_recv()

    def arrived_mate(buf, sems, p):
        to_mate(buf.at[p], buf.at[p], sems.at[p], sems.at[p], p).wait_recv()

    load_tok.wait()

    def spread(z, go_up, go_down):
        @pl.when(go_up & (at_line + 1 < line))
        def _():
            up_copy(z).start()

        @pl.when(go_down & (at_line >= 1))
        def _():
            down_copy(z).start()

        each(1, side, lambda s: side_copy(z, s).start())

    spread(at_line, True, True)
    each(1, n, lambda s: gate_copy(s).start())
    au_all[me] = au_ref[0]
    gate_recv[me] = gexp[me, 0:8]

    load_gw.wait()
    load_uw.wait()
    load_dw.wait()

    def expert_block(src):
        x = tok_all[src]
        g = dot_nt(x, gw[...])
        u = dot_nt(x, uw[...])
        h = (g / (1.0 + jnp.exp(-g)) * u).astype(BF16)
        hid_all[src] = h
        low_t = dot_nt(ad_ref[0], h).astype(BF16)
        low = dot_nt(h, ad_ref[0]).astype(BF16)
        out = (dot(h, dw[...]) + dot(low, au_ref[0])).astype(BF16)
        return low_t, out

    def low_grads():
        each(1, n, lambda s: arrived(au_all, au_r, source(s)))
        low_grad = dot_nt(au_all[...].reshape(n * rank, width), og_ref[...])
        low_grad = low_grad * gexp[...].reshape(n * rank, rows)
        lg_send[...] = low_grad.astype(BF16).reshape(n, rank, rows)
        lg_recv[me] = lg_send[me]
        each(1, n, lambda s: lg_copy(s).start())

    def on_line(z):
        return (z >= 0) & (z < line)

    def relay(k):
        for sign in (-1, 1):
            z = at_line + sign * k

            @pl.when((k >= 1) & on_line(z))
            def _():
                arrived(tok_all, tok_r, z * side + at_side)
                spread(z, sign < 0, sign > 0)

    def work(k, j):
        s = j // 2
        sign = 1 - 2 * lax.rem(j, 2)
        far = k - jnp.minimum(s, 1)
        z = at_line + sign * far
        x = lax.rem(at_side + s, side)
        src = z * side + x

        @pl.when(on_line(z) & (far >= 0) & ((far > 0) | (sign > 0)))
        def _():
            @pl.when(s > 0)
            def _():
                arrived(tok_all, tok_r, src)

            @pl.when(src != me)
            def _():
                arrived(gate_recv, gate_r, src)

            low_t, out = expert_block(src)
            row = gate_recv[src, 0:1]
            column = jnp.sum(jnp.where(eye, row, 0.0), axis=1, keepdims=True)
            term = (out.astype(F32) * column).astype(BF16)

            @pl.when(s > 0)
            def _():
                out_send[src] = term

            @pl.when(s == 0)
            def _():
                pair_recv[src] = term

            @pl.when(src == me)
            def _():
                rk_recv[me] = low_t

            @pl.when(src != me)
            def _():
                rk_send[src] = low_t
                rk_copy(src).start()

            @pl.when(s > 0)
            def _():
                pair_copy(z, x).start()

    def pair_sum(z):
        def wait_pair(s):
            arrived(pair_recv, pair_r, z * side + lax.rem(at_side + s, side))

        each(1, side, wait_pair)

        def add(x, total):
            return total + pair_recv[z * side + x].astype(F32)

        return lax.fori_loop(1, side, add, pair_recv[z * side].astype(F32))

    def combine(k):
        for sign in (-1, 1):
            z = at_line + sign * (k - 2)

            @pl.when((k >= 3) & on_line(z))
            def _():
                line_send[z] = pair_sum(z).astype(BF16)
                line_copy(z).start()

    def grads():
        each(1, n, lambda s: arrived(lg_recv, lg_r, source(s)))

        def add_gin(src, total):
            return total + dot(lg_recv[src], hid_all[src])

        gin_all[rep] = lax.fori_loop(0, n, add_gin, jnp.zeros(gin_all.shape[1:], F32))

        each(1, n, lambda s: arrived(rk_recv, rk_r, source(s)))
        low_w = (rk_recv[...].astype(F32) * gexp[...]).astype(BF16).reshape(n * rank, rows)
        gp = dot(low_w, og_ref[...])
        gp_send[...] = gp.astype(BF16).reshape(n, rank, width)
        each(1, nd, lambda s: gin_copy(s).start())
        gp_recv[me] = gp_send[me]
        each(1, n, lambda s: gp_copy(peer(s)).start())

    def step(k):
        relay(k)
        pl.when(k == 2)(lambda: each(1, n, lambda s: au_copy(s).start()))
        each(0, 2 * side, lambda j: work(k, j))
        pl.when(k == line)(low_grads)
        pl.when(k == line + 1)(grads)
        combine(k)

    each(0, line + 2, step)

    acc[...] = pair_sum(at_line)
    each(1, n, lambda s: arrived(gp_recv, gp_r, source(s)))
    gout_all[rep] = jnp.sum(gp_recv[...].astype(F32), axis=0)
    each(1, nd, lambda s: gout_copy(s).start())

    def finish(t):
        z = lax.rem(at_line + t, line)
        arrived(line_recv, line_r, z)
        acc[...] += line_recv[z].astype(F32)

    each(1, line, finish)
    mixed_ref[...] = acc[...].astype(BF16)

    each(1, nd, lambda s: arrived_mate(gin_all, gin_r, mate(s)))
    gin_ref[0] = jnp.sum(gin_all[...], axis=0).astype(BF16)
    each(1, nd, lambda s: arrived_mate(gout_all, gout_r, mate(s)))
    gout_ref[0] = jnp.sum(gout_all[...], axis=0).astype(BF16)

    def drain(s):
        au_copy(s).wait_send()
        gate_copy(s).wait_send()
        lg_copy(s).wait_send()
        p = peer(s)
        rk_copy(p).wait_send()
        gp_copy(p).wait_send()

    each(1, n, drain)

    def drain_line(z):
        @pl.when((z <= at_line) & (at_line + 1 < line))
        def _():
            up_copy(z).wait_send()

        @pl.when((z >= at_line) & (at_line >= 1))
        def _():
            down_copy(z).wait_send()

        def drain_side(s):
            side_copy(z, s).wait_send()
            pair_copy(z, lax.rem(at_side + s, side)).wait_send()

        each(1, side, drain_side)

        @pl.when(z != at_line)
        def _():
            line_copy(z).wait_send()

    each(0, line, drain_line)

    def drain_mates(s):
        gin_copy(s).wait_send()
        gout_copy(s).wait_send()

    each(1, nd, drain_mates)


def hand_over(a_ref, b_ref, c_ref, x_ref, y_ref, z_ref):
    x_ref[...] = a_ref[...]
    y_ref[...] = b_ref[...]
    z_ref[...] = c_ref[...]


def shards(
    n,
    nd,
    tokens,
    chosen_expert_index,
    router_gate_weight,
    output_gradient,
    gate_weight_matrix,
    up_weight,
    down_weight,
    adapter_down_maps,
    adapter_up_maps,
):
    rows, width = tokens.shape
    rank, hidden = adapter_down_maps.shape[1:]
    line = 4 if n % 4 == 0 else n
    vmem = pl.BlockSpec(memory_space=pltpu.VMEM)
    anywhere = pl.BlockSpec(memory_space=pl.ANY)
    dma = pltpu.SemaphoreType.DMA
    results = pl.pallas_call(
        functools.partial(kernel, n, nd),
        out_shape=(
            jax.ShapeDtypeStruct((rows, width), BF16),
            jax.ShapeDtypeStruct((1, rank, hidden), BF16),
            jax.ShapeDtypeStruct((1, rank, width), BF16),
        ),
        in_specs=[anywhere, vmem, vmem, vmem, anywhere, anywhere, anywhere, vmem, vmem],
        out_specs=(vmem, vmem, vmem),
        scratch_shapes=[
            pltpu.VMEM((n, rows, width), BF16),
            pltpu.VMEM((hidden, width), BF16),
            pltpu.VMEM((hidden, width), BF16),
            pltpu.VMEM((hidden, width), BF16),
            pltpu.VMEM((n, rows, hidden), BF16),
            pltpu.VMEM((n, rows, width), BF16),
            pltpu.VMEM((n, rows, width), BF16),
            pltpu.VMEM((line, rows, width), BF16),
            pltpu.VMEM((line, rows, width), BF16),
            pltpu.VMEM((n, 8, rows), F32),
            pltpu.VMEM((n, rank, width), BF16),
            pltpu.VMEM((n, rank, rows), BF16),
            pltpu.VMEM((n, rank, rows), BF16),
            pltpu.VMEM((n, rank, rows), BF16),
            pltpu.VMEM((n, rank, rows), BF16),
            pltpu.VMEM((n, rank, rows), F32),
            pltpu.VMEM((n, rank, width), BF16),
            pltpu.VMEM((n, rank, width), BF16),
            pltpu.VMEM((nd, rank, hidden), F32),
            pltpu.VMEM((nd, rank, width), F32),
            pltpu.VMEM((rows, width), F32),
            dma((4,)),
        ]
        + [dma((line,))] * 2
        + [dma((n,))] * 12
        + [dma((line,))] * 2
        + [dma((n,))] * 2
        + [dma((nd,))] * 4,
        compiler_params=pltpu.CompilerParams(
            collective_id=0, has_side_effects=True, vmem_limit_bytes=60 * 1024 * 1024
        ),
    )(
        tokens,
        chosen_expert_index.T,
        router_gate_weight.T,
        output_gradient,
        jnp.swapaxes(gate_weight_matrix, 1, 2),
        jnp.swapaxes(up_weight, 1, 2),
        down_weight,
        adapter_down_maps,
        adapter_up_maps,
    )
    return pl.pallas_call(
        hand_over,
        out_shape=tuple(jax.ShapeDtypeStruct(r.shape, r.dtype) for r in results),
        in_specs=[vmem] * 3,
        out_specs=(vmem,) * 3,
    )(*results)


def solution(mesh):
    return jax.shard_map(
        functools.partial(shards, mesh.shape["expert"], mesh.shape["dp"]),
        mesh=mesh,
        in_specs=(
            P(("dp", "expert"), None),
            P(("dp", "expert"), None),
            P(("dp", "expert"), None),
            P(("dp", "expert"), None),
            P("expert", None, None),
            P("expert", None, None),
            P("expert", None, None),
            P("expert", None, None),
            P("expert", None, None),
        ),
        out_specs=(P(("dp", "expert"), None), P("expert", None, None), P("expert", None, None)),
        check_vma=False,
    )
```
